32 devices in a mesh: district: 4 (over y, core), sub: 8 (over z, x).
Axes of the slice: x: 2, y: 2, z: 4, core: 2. Of those that a mesh axis runs over, the one named last changes fastest.
Arguments:
- cost_terms: bfloat16 [8, 512, 768], P('district', 'sub'), may hold values from -6 to 6
- neighbours: int32 [8, 512, 4], P('district', 'sub'), may hold values from 0 to 511, as said below
- relayout: int32 [8, 512], P('district'), may hold values from 0 to 511, as said below
- ownership: int32 [8, 512], P('district', 'sub'), may hold values from 0 to 31
- capacity: float32 [16, 48], replicated, may hold values from -67.88225 to 67.88225
- coupling: bfloat16 [8, 768, 192], P('district'), may hold values from -0.21875 to 0.21875
- solve_factor: bfloat16 [8, 768, 768], P('district')
Outputs:
- control_plan: float32 [8, 512, 768], P('district', 'sub')
- flow_prices: float32 [8, 512, 192], P('district', 'sub')
- reservoir_duals: float32 [16, 48], replicated
The draws below stay inside these ranges and needn't reach their ends.
Inputs may be any that keep to these rules, and one draw needn't show every extreme that they name: `neighbours`: each entry lies within 16 of its own balanced position and differs from it. `relayout`: each row is a permutation; of the subsystems at geographic positions s * 64 to (s + 1) * 64 - 1, exactly 8 go to balanced positions j * 64 to (j + 1) * 64 - 1, for every s and j. `ownership`: values of 16 or more mean that the subsystem draws from no reservoir.
All inputs are finite; a program needn't handle non-finite values.
Results may differ from the reference program's by a relative error of at most 0.018.
Values may be sent and summed in bfloat16 or wider, within the bound.
A program may use at most 64 MiB of HBM per device.

```python
import math
import jax
import jax.numpy as jnp
from jax import lax

HORIZON = 48
UNKNOWNS = 768
INTERFACE = 192
SUB_DEV = 64
DISTRICTS = 8
SUB_DIST = 512
PEER_SHARE = 8
REACH_SPAN = 16
LINK_COUNT = 4
RESERVOIRS = 16
RESERVOIR_LOAD = 128
OUTER_ITERS = 2
INNER_ITERS = 4


def draw_neighbours(key, part):
    picks = jax.random.randint(key, (DISTRICTS, SUB_DIST, LINK_COUNT), 0, 2 * REACH_SPAN)
    offsets = picks - REACH_SPAN + (picks >= REACH_SPAN).astype(jnp.int32)
    places = jnp.arange(SUB_DIST, dtype=jnp.int32)[None, :, None]
    target = places + offsets
    target = jnp.where((target < 0) | (target >= SUB_DIST), places - offsets, target)
    return target.astype(jnp.int32)


def draw_relayout(key, part):
    first_key = jax.random.fold_in(key, 11)
    second_key = jax.random.fold_in(key, 23)
    groups = SUB_DIST // SUB_DEV
    base = jnp.tile(jnp.arange(SUB_DEV, dtype=jnp.int32)[None, :], (DISTRICTS * groups, 1))
    source_perm = jax.random.permutation(first_key, base, axis=1, independent=True).reshape(DISTRICTS, groups, SUB_DEV)
    target_perm = jax.random.permutation(second_key, base, axis=1, independent=True).reshape(DISTRICTS, groups, SUB_DEV)
    dest_block = source_perm // PEER_SHARE
    within = source_perm % PEER_SHARE
    sources = jnp.arange(groups, dtype=jnp.int32)[None, :, None]
    slot_index = sources * PEER_SHARE + within
    district_rows = jnp.arange(DISTRICTS, dtype=jnp.int32)[:, None, None]
    target = dest_block * SUB_DEV + target_perm[district_rows, dest_block, slot_index]
    return target.reshape(DISTRICTS, SUB_DIST).astype(jnp.int32)


def draw_solve_factor(key, part):
    first_key = jax.random.fold_in(key, 5)
    second_key = jax.random.fold_in(key, 7)
    diagonal = jnp.exp(jax.random.uniform(first_key, (DISTRICTS, UNKNOWNS), jnp.float32, jnp.log(0.5), jnp.log(2.0)))
    spread = jax.random.normal(second_key, (DISTRICTS, UNKNOWNS, UNKNOWNS), jnp.float32) * (0.5 / UNKNOWNS ** 0.5)
    matrix = spread + diagonal[:, :, None] * jnp.eye(UNKNOWNS, dtype=jnp.float32)[None, :, :]
    return matrix.astype(jnp.bfloat16)


def set_ends(entries, own_key, low, high):
    dims = entries.shape
    index_at = [jax.random.randint(jax.random.fold_in(own_key, axis), (), 0, dims[axis]) for axis in range(len(dims))]
    entries = entries.at[tuple(index_at)].set(low)
    longest = dims.index(max(dims))
    index_at[longest] = (index_at[longest] + 1) % dims[longest]
    return entries.at[tuple(index_at)].set(high)


def shard_levels(key, shape, pieces, least, high):
    factor_of, own = 1.0, jax.random.fold_in(key, 6)
    for position, parts in pieces:
        heights = jnp.exp(jax.random.uniform(jax.random.fold_in(own, position), (parts,), jnp.float32, least / len(pieces), high / len(pieces)))
        factor_of = factor_of * jnp.repeat(heights, shape[position] // parts).reshape([-1 if axis == position else 1 for axis in range(len(shape))])
    return factor_of


def normal_values(stream_key, shape, scale, limit, split=(), held_as=jnp.bfloat16):
    values = scale * jax.random.normal(stream_key, shape, jnp.float32)
    if split:
        values = values * shard_levels(stream_key, shape, split, -0.22, 0.18)
    return jnp.clip(values, -limit, limit).astype(held_as)


def setup_inputs(seed: int = 0) -> dict:
    seeds = jax.random.split(jax.random.key(seed), 8)
    return {
        "cost_terms": normal_values(seeds[0], (DISTRICTS, SUB_DIST, UNKNOWNS), 1.0, 6.0, ((0, 4), (1, 8))),
        "neighbours": draw_neighbours(jax.random.fold_in(seeds[7], 71), 0),
        "relayout": draw_relayout(jax.random.fold_in(seeds[7], 71), 0),
        "ownership": set_ends(jax.random.randint(seeds[3], (DISTRICTS, SUB_DIST), 0, 2 * RESERVOIRS), jax.random.fold_in(seeds[3], 1), 0, (2 * RESERVOIRS) - 1).astype(jnp.int32),
        "capacity": normal_values(seeds[4], (RESERVOIRS, HORIZON), (RESERVOIR_LOAD ** 0.5), 67.88225, (), jnp.float32),
        "coupling": normal_values(seeds[5], (DISTRICTS, UNKNOWNS, INTERFACE), UNKNOWNS ** -0.5, 0.21875, ((0, 4),)),
        "solve_factor": draw_solve_factor(jax.random.fold_in(seeds[7], 71), 0),
    }


price_step = 0.3
reserve_step = 1.0

def neighbour_mean(values, links):
    district_rows = jnp.arange(values.shape[0], dtype=jnp.int32)[:, None]
    running = jnp.zeros(links.shape[:2] + values.shape[2:], jnp.float32)
    for which in range(LINK_COUNT):
        running = running + values[district_rows, links[:, :, which]].astype(jnp.float32)
    return running / LINK_COUNT

def reference(cost_terms, neighbours, relayout, ownership, capacity, coupling, solve_factor):
    district_rows = jnp.arange(DISTRICTS, dtype=jnp.int32)[:, None]
    inverse = jnp.argsort(relayout, axis=1, stable=True).astype(jnp.int32)
    balanced_costs = cost_terms[district_rows, inverse]
    owner_slot = jnp.where(ownership < RESERVOIRS, ownership, RESERVOIRS).astype(jnp.int32)
    flow_prices = jnp.zeros((DISTRICTS, SUB_DIST, INTERFACE), jnp.float32)
    reserve_duals = jnp.zeros((RESERVOIRS, HORIZON), jnp.float32)
    dual_scale = reserve_step / math.sqrt(RESERVOIR_LOAD)
    highest = lax.Precision.HIGHEST
    coupling_wide = coupling.astype(jnp.float32)
    factor_wide = solve_factor.astype(jnp.float32)
    plan_now = None
    flow_now = None
    for outer_step in range(OUTER_ITERS):
        for inner_step in range(INNER_ITERS):
            padded_duals = jnp.concatenate([reserve_duals, jnp.zeros((1, HORIZON), jnp.float32)], axis=0)
            boundary = padded_duals[owner_slot]
            boundary = jnp.concatenate([boundary, jnp.zeros((DISTRICTS, SUB_DIST, INTERFACE - HORIZON), jnp.float32)], axis=2)
            price_term = (flow_prices - neighbour_mean(flow_prices, neighbours) + boundary).astype(jnp.bfloat16)
            gradient = (balanced_costs.astype(jnp.float32) + jnp.einsum('dsf,dzf->dsz', price_term.astype(jnp.float32), coupling_wide, precision=highest)).astype(jnp.bfloat16)
            plan_now = -jnp.einsum('dsz,dzw->dsw', gradient.astype(jnp.float32), factor_wide, precision=highest)
            plan_rounded = plan_now.astype(jnp.bfloat16)
            flow_now = jnp.einsum('dsz,dzf->dsf', plan_rounded.astype(jnp.float32), coupling_wide, precision=highest).astype(jnp.bfloat16)
            flow_prices = flow_prices + price_step * (flow_now.astype(jnp.float32) - neighbour_mean(flow_now, neighbours))
        draws = jax.ops.segment_sum(flow_now[:, :, :HORIZON].astype(jnp.float32).reshape(-1, HORIZON), owner_slot.reshape(-1), num_segments=RESERVOIRS + 1)[:RESERVOIRS]
        reserve_duals = reserve_duals + (draws - capacity) * dual_scale
    control_plan = plan_now[district_rows, relayout]
    return (control_plan, flow_prices, reserve_duals)
```

```python
import functools
import math

import jax
import jax.numpy as jnp
from jax import lax
from jax.experimental import pallas as pl
from jax.experimental.pallas import tpu as pltpu
from jax.sharding import PartitionSpec as P

REACH_SPAN = 16
LINK_COUNT = 4
RESERVOIRS = 16
OUTER_ITERS = 2
INNER_ITERS = 4
HALO = 2 * REACH_SPAN
LANES = 128

price_step = 0.3
reserve_step = 1.0

F32 = jnp.float32
BF16 = jnp.bfloat16
MESH = pl.DeviceIdType.MESH


def each(count, body):
    if count <= 8:
        for index in range(count):
            body(index)
    else:
        lax.fori_loop(0, count, lambda index, carry: (body(index), carry)[1], 0)


def mm(a, b):
    return jnp.dot(a, b, preferred_element_type=F32)


def contract(a, b, dim):
    return lax.dot_general(a, b, (((dim,), (dim,)), ((), ())), preferred_element_type=F32)


def kernel(
    dual_scale, costs_ref, meta_ref, relayout_ref, capacity_ref, coupling_hbm, factor_hbm,
    plan_ref, prices_ref, duals_ref,
    coupling, factor, meta, links, owners, gathered, base, state, flow, total, spread, weight,
    match, match_t, select, own_links, duals, draws, arrived,
    local_sem, meta_send, meta_recv, flow_send, flow_recv, draw_send, draw_recv,
):
    districts, rows, unknowns = costs_ref.shape
    interface = coupling.shape[2]
    horizon = capacity_ref.shape[1]
    group = relayout_ref.shape[1]
    sub_count = lax.axis_size("sub")
    district_count = lax.axis_size("district")
    me = lax.axis_index("sub")
    my_district = lax.axis_index("district")
    block = 2 * rows
    window = block + 2 * HALO
    blocks = group // block

    loads = []
    for d in range(districts):
        loads.append(
            (
                pltpu.make_async_copy(factor_hbm.at[d], factor.at[d], local_sem.at[2 * d]),
                pltpu.make_async_copy(coupling_hbm.at[d], coupling.at[d], local_sem.at[2 * d + 1]),
            )
        )
        for load in loads[-1]:
            load.start()

    barrier = pltpu.get_barrier_semaphore()
    for step in range(1, sub_count):
        pl.semaphore_signal(
            barrier, inc=1, device_id={"sub": lax.rem(me + step, sub_count)}, device_id_type=MESH
        )
    for step in range(1, district_count):
        pl.semaphore_signal(
            barrier,
            inc=1,
            device_id={"district": lax.rem(my_district + step, district_count)},
            device_id_type=MESH,
        )

    mine = pl.ds(pl.multiple_of(me * rows, rows), rows)
    for d in range(districts):
        for load in loads[d]:
            load.wait()
        first_plan = -mm(costs_ref[d], factor[d])
        gathered[d, mine, :] = mm(first_plan.astype(BF16), coupling[d]).astype(BF16)

    pl.semaphore_wait(barrier, sub_count - 1 + district_count - 1)
    sends = []
    for step in range(1, sub_count):
        target = lax.rem(me + step, sub_count)
        sends.append(
            pltpu.make_async_remote_copy(
                src_ref=meta_ref,
                dst_ref=meta.at[me],
                send_sem=meta_send.at[step],
                recv_sem=meta_recv.at[me],
                device_id={"sub": target},
                device_id_type=MESH,
            )
        )
        sends[-1].start()
    for step in range(1, sub_count):
        target = lax.rem(me + step, sub_count)
        sends.append(
            pltpu.make_async_remote_copy(
                src_ref=gathered.at[:, mine, :],
                dst_ref=gathered.at[:, mine, :],
                send_sem=flow_send.at[step],
                recv_sem=flow_recv.at[me],
                device_id={"sub": target},
                device_id_type=MESH,
            )
        )
        sends[-1].start()

    for d in range(districts):
        narrow = mm(factor[d], coupling[d]).astype(BF16)
        weight[d] = (-contract(coupling[d], narrow, 0)).astype(BF16)

    wide = rows + 2 * HALO
    for d in range(districts):
        moved = meta_ref[(LINK_COUNT + 1) * districts + d : (LINK_COUNT + 1) * districts + d + 1, :]
        place = lax.broadcasted_iota(jnp.int32, (group, rows), 0)
        select[d] = jnp.where(place == moved, 1.0, 0.0).astype(F32).T.astype(BF16)
        column = lax.broadcasted_iota(jnp.int32, (wide, rows), 0)
        row = lax.broadcasted_iota(jnp.int32, (wide, rows), 1)
        table = jnp.where(column == row + HALO, 1.0, 0.0)
        for k in range(LINK_COUNT):
            link = meta_ref[LINK_COUNT * d + k : LINK_COUNT * d + k + 1, :] - (me * rows - HALO)
            table = table - jnp.where(column == link, 1.0 / LINK_COUNT, 0.0)
        own_links[d] = table.T.astype(BF16)

    duals[...] = jnp.zeros_like(duals)
    duals[:, :horizon] = capacity_ref[...]
    capacity = duals[...]
    flow[...] = jnp.zeros_like(flow)
    links[...] = jnp.full_like(links, -window * 4)

    meta[me] = meta_ref[...]
    for step in range(1, sub_count):
        source = lax.rem(me + step, sub_count)
        pltpu.make_async_remote_copy(
            src_ref=meta_ref,
            dst_ref=meta.at[source],
            send_sem=meta_send.at[step],
            recv_sem=meta_recv.at[source],
            device_id={"sub": source},
            device_id_type=MESH,
        ).wait_recv()
    for source in range(sub_count):
        piece = meta[source]
        links[:, HALO + source * rows : HALO + (source + 1) * rows] = piece[: LINK_COUNT * districts]
        owners[:, source * rows : (source + 1) * rows] = piece[
            LINK_COUNT * districts : (LINK_COUNT + 1) * districts
        ]
    for d in range(districts):
        own = owners[d : d + 1, :]
        hit = jnp.where(
            lax.broadcasted_iota(jnp.int32, (RESERVOIRS, group), 0) == own, 1.0, 0.0
        ).astype(F32)
        match_t[d] = hit.astype(BF16)
        match[d] = hit.T.astype(BF16)

        def build(b, d=d):
            start = b * block if isinstance(b, int) else pl.multiple_of(b * block, block)
            column = lax.broadcasted_iota(jnp.int32, (window, window), 0)
            row = lax.broadcasted_iota(jnp.int32, (window, window), 1)
            table = jnp.where(column == row, 1.0, 0.0)
            for k in range(LINK_COUNT):
                at = LINK_COUNT * d + k
                link = links[at : at + 1, pl.ds(start, window)] - (start - HALO)
                table = table - jnp.where(column == link, 1.0 / LINK_COUNT, 0.0)
            table = table.T.astype(BF16)
            spread[d, b] = mm(table[HALO : HALO + block], table).astype(BF16)

        each(blocks, build)

    for step in range(1, sub_count):
        source = lax.rem(me + step, sub_count)
        pltpu.make_async_remote_copy(
            src_ref=gathered.at[:, mine, :],
            dst_ref=gathered.at[:, pl.ds(pl.multiple_of(source * rows, rows), rows), :],
            send_sem=flow_send.at[step],
            recv_sem=flow_recv.at[source],
            device_id={"sub": source},
            device_id_type=MESH,
        ).wait_recv()

    def at_block(b, extra=0, size=block):
        return pl.ds(b * block + extra, size)

    for d in range(districts):
        def permute(b, d=d):
            place = lax.broadcasted_iota(jnp.int32, (block, group), 0) + b * block
            chosen = jnp.where(place == relayout_ref[d : d + 1, :], 1.0, 0.0).astype(BF16)
            moved = mm(chosen, gathered[d])
            base[d, at_block(b), :] = moved
            flow[d, at_block(b, HALO), :] = moved.astype(BF16)

        each(blocks, permute)

    own_window = pl.ds(pl.multiple_of(me * rows, rows), wide)
    for d in range(districts):
        total[d] = flow[d, own_window, :].astype(F32)

        def begin(b, d=d):
            state[d, at_block(b), :] = price_step * mm(spread[d, b], flow[d, at_block(b, 0, window), :])

        each(blocks, begin)

    def forward():
        for d in range(districts):
            def one(b, d=d):
                price = state[d, at_block(b), :].astype(BF16)
                flow[d, at_block(b, HALO), :] = (base[d, at_block(b), :] + mm(price, weight[d])).astype(BF16)

            each(blocks, one)
            total[d] += flow[d, own_window, :].astype(F32)

    def backward():
        for d in range(districts):
            def one(b, d=d):
                state[d, at_block(b), :] += price_step * mm(
                    spread[d, b], flow[d, at_block(b, 0, window), :]
                )

            each(blocks, one)

    def inner(step, carry):
        forward()
        backward()
        return carry

    def send_draws(outer):
        drawn = mm(match_t[0], flow[0, HALO : HALO + group, :])
        for d in range(1, districts):
            drawn = drawn + mm(match_t[d], flow[d, HALO : HALO + group, :])
        draws[outer] = drawn[:, :LANES]
        copies = []
        for step in range(1, district_count):
            copies.append(
                pltpu.make_async_remote_copy(
                    src_ref=draws.at[outer],
                    dst_ref=arrived.at[outer, step],
                    send_sem=draw_send.at[outer, step],
                    recv_sem=draw_recv.at[outer, step],
                    device_id={"district": lax.rem(my_district + step, district_count)},
                    device_id_type=MESH,
                )
            )
            copies[-1].start()
        return copies

    def take_draws(outer, copies):
        drawn = draws[outer]
        for step in range(1, district_count):
            copies[step - 1].wait()
            drawn = drawn + arrived[outer, step]
        lane = lax.broadcasted_iota(jnp.int32, drawn.shape, 1)
        return jnp.where(lane < horizon, (drawn - capacity) * dual_scale, 0.0)

    lax.fori_loop(1, INNER_ITERS - 1, inner, 0)
    forward()
    copies = send_draws(0)
    backward()
    moved = take_draws(0, copies)
    for outer in range(1, OUTER_ITERS):
        duals[...] = moved if outer == 1 else duals[...] + moved
        high = moved.astype(BF16)
        low = (moved - high.astype(F32)).astype(BF16)
        for d in range(districts):
            state[d, :, :LANES] += mm(match[d], high) + mm(match[d], low)
        lax.fori_loop(0, INNER_ITERS - 1, inner, 0)
        forward()
        copies = send_draws(outer)
        if outer < OUTER_ITERS - 1:
            backward()
        else:
            for d in range(districts):
                chosen = mm(select[d], state[d].astype(BF16)).astype(BF16)
                gradient = costs_ref[d].astype(F32) + contract(chosen, coupling[d], 1)
                plan_ref[d] = -mm(gradient.astype(BF16), factor[d])
                summed = total[d]
                high = summed.astype(BF16)
                low = (summed - high.astype(F32)).astype(BF16)
                prices_ref[d] = price_step * (mm(own_links[d], high) + mm(own_links[d], low))
        moved = take_draws(outer, copies)
    duals_ref[...] = (duals[...] + moved)[:, :horizon]
    for send in sends:
        send.wait_send()


def on_device(cost_terms, neighbours, relayout, ownership, capacity, coupling, solve_factor):
    districts, rows, unknowns = cost_terms.shape
    interface = coupling.shape[2]
    group = relayout.shape[1]
    sub_count = lax.axis_size("sub")
    district_count = lax.axis_size("district")
    load_count = districts * district_count * group // (2 * RESERVOIRS)
    dual_scale = reserve_step / math.sqrt(load_count)
    own_moves = lax.dynamic_slice_in_dim(relayout, lax.axis_index("sub") * rows, rows, 1)
    meta = jnp.concatenate(
        [neighbours.transpose(0, 2, 1).reshape(districts * LINK_COUNT, rows), ownership, own_moves], axis=0
    )
    meta = jnp.pad(meta, ((0, -meta.shape[0] % 8), (0, 0)))
    block = 2 * rows
    blocks = group // block
    window = block + 2 * HALO
    vmem = pl.BlockSpec(memory_space=pltpu.VMEM)
    hbm = pl.BlockSpec(memory_space=pl.ANY)
    dma = pltpu.SemaphoreType.DMA
    return pl.pallas_call(
        functools.partial(kernel, dual_scale),
        name="districts",
        out_shape=(
            jax.ShapeDtypeStruct((districts, rows, unknowns), F32),
            jax.ShapeDtypeStruct((districts, rows, interface), F32),
            jax.ShapeDtypeStruct(capacity.shape, F32),
        ),
        in_specs=[vmem, vmem, vmem, vmem, hbm, hbm],
        out_specs=(vmem, vmem, vmem),
        scratch_shapes=[
            pltpu.VMEM(coupling.shape, BF16),
            pltpu.VMEM(solve_factor.shape, BF16),
            pltpu.VMEM((sub_count,) + meta.shape, jnp.int32),
            pltpu.VMEM((districts * LINK_COUNT, group + 2 * HALO), jnp.int32),
            pltpu.VMEM((districts, group), jnp.int32),
            pltpu.VMEM((districts, group, interface), BF16),
            pltpu.VMEM((districts, group, interface), F32),
            pltpu.VMEM((districts, group, interface), F32),
            pltpu.VMEM((districts, group + 2 * HALO, interface), BF16),
            pltpu.VMEM((districts, rows + 2 * HALO, interface), F32),
            pltpu.VMEM((districts, blocks, block, window), BF16),
            pltpu.VMEM((districts, interface, interface), BF16),
            pltpu.VMEM((districts, group, RESERVOIRS), BF16),
            pltpu.VMEM((districts, RESERVOIRS, group), BF16),
            pltpu.VMEM((districts, rows, group), BF16),
            pltpu.VMEM((districts, rows, rows + 2 * HALO), BF16),
            pltpu.VMEM((RESERVOIRS, LANES), F32),
            pltpu.VMEM((OUTER_ITERS, RESERVOIRS, LANES), F32),
            pltpu.VMEM((OUTER_ITERS, district_count, RESERVOIRS, LANES), F32),
            dma((2 * districts,)),
            dma((sub_count,)),
            dma((sub_count,)),
            dma((sub_count,)),
            dma((sub_count,)),
            dma((OUTER_ITERS, district_count)),
            dma((OUTER_ITERS, district_count)),
        ],
        compiler_params=pltpu.CompilerParams(
            collective_id=0, has_side_effects=True, vmem_limit_bytes=60 * 1024 * 1024
        ),
    )(cost_terms, meta, relayout, capacity, coupling, solve_factor)


def solution(mesh):
    placed = (
        P("district", "sub", None),
        P("district", "sub", None),
        P("district", None),
        P("district", "sub"),
        P(),
        P("district", None, None),
        P("district", None, None),
    )
    return jax.shard_map(
        on_device,
        mesh=mesh,
        in_specs=placed,
        out_specs=(P("district", "sub", None), P("district", "sub", None), P()),
        check_vma=False,
    )
```

```python
import functools
import math

import jax
import jax.numpy as jnp
from jax import lax
from jax.experimental import pallas as pl
from jax.experimental.pallas import tpu as pltpu
from jax.sharding import PartitionSpec as P

REACH_SPAN = 16
LINK_COUNT = 4
RESERVOIRS = 16
OUTER_ITERS = 2
INNER_ITERS = 4
HALO = 2 * REACH_SPAN
LANES = 128

price_step = 0.3
reserve_step = 1.0

F32 = jnp.float32
BF16 = jnp.bfloat16
MESH = pl.DeviceIdType.MESH


def each(count, body):
    if count <= 8:
        for index in range(count):
            body(index)
    else:
        lax.fori_loop(0, count, lambda index, carry: (body(index), carry)[1], 0)


def mm(a, b):
    return jnp.dot(a, b, preferred_element_type=F32)


def contract(a, b, dim):
    return lax.dot_general(a, b, (((dim,), (dim,)), ((), ())), preferred_element_type=F32)


def kernel(
    dual_scale, costs_ref, near_ref, owner_ref, relayout_ref, capacity_ref, coupling_hbm, factor_hbm,
    plan_ref, prices_ref, duals_ref,
    coupling, factor, near, owned, links, owners, gathered, base, state, flow, total, spread, weight,
    match, match_t, select, own_links, duals, draws, arrived,
    local_sem, near_send, near_recv, owner_send, owner_recv, flow_send, flow_recv, draw_send, draw_recv,
):
    districts, rows, unknowns = costs_ref.shape
    interface = coupling.shape[1]
    horizon = capacity_ref.shape[1]
    group = relayout_ref.shape[1]
    sub_count = lax.axis_size("sub")
    district_count = lax.axis_size("district")
    me = lax.axis_index("sub")
    my_district = lax.axis_index("district")
    block = 2 * rows
    window = block + 2 * HALO
    blocks = group // block

    loads = []
    for d in range(districts):
        loads.append(
            (
                pltpu.make_async_copy(factor_hbm.at[d], factor.at[d], local_sem.at[2 * d]),
                pltpu.make_async_copy(coupling_hbm.at[d], coupling.at[d], local_sem.at[2 * d + 1]),
            )
        )
        for load in loads[-1]:
            load.start()

    barrier = pltpu.get_barrier_semaphore()
    for step in range(1, sub_count):
        pl.semaphore_signal(
            barrier, inc=1, device_id={"sub": lax.rem(me + step, sub_count)}, device_id_type=MESH
        )
    for step in range(1, district_count):
        pl.semaphore_signal(
            barrier,
            inc=1,
            device_id={"district": lax.rem(my_district + step, district_count)},
            device_id_type=MESH,
        )

    mine = pl.ds(pl.multiple_of(me * rows, rows), rows)
    for d in range(districts):
        for load in loads[d]:
            load.wait()
        first_plan = -mm(costs_ref[d], factor[d])
        gathered[d, mine, :] = contract(first_plan.astype(BF16), coupling[d], 1).astype(BF16)

    pl.semaphore_wait(barrier, sub_count - 1 + district_count - 1)
    sends = []
    for step in range(1, sub_count):
        target = lax.rem(me + step, sub_count)
        for source_ref, place_ref, send_sem, recv_sem in (
            (near_ref, near, near_send, near_recv),
            (owner_ref, owned, owner_send, owner_recv),
        ):
            sends.append(
                pltpu.make_async_remote_copy(
                    src_ref=source_ref,
                    dst_ref=place_ref.at[me],
                    send_sem=send_sem.at[step],
                    recv_sem=recv_sem.at[me],
                    device_id={"sub": target},
                    device_id_type=MESH,
                )
            )
            sends[-1].start()
    for step in range(1, sub_count):
        target = lax.rem(me + step, sub_count)
        sends.append(
            pltpu.make_async_remote_copy(
                src_ref=gathered.at[:, mine, :],
                dst_ref=gathered.at[:, mine, :],
                send_sem=flow_send.at[step],
                recv_sem=flow_recv.at[me],
                device_id={"sub": target},
                device_id_type=MESH,
            )
        )
        sends[-1].start()

    for d in range(districts):
        narrow = mm(coupling[d], factor[d]).astype(BF16)
        weight[d] = (-contract(narrow, coupling[d], 1)).astype(BF16)

    wide = rows + 2 * HALO
    for d in range(districts):
        pick = lax.broadcasted_iota(jnp.int32, (rows, group), 1) == (
            lax.broadcasted_iota(jnp.int32, (rows, group), 0) + me * rows
        )
        pick = jnp.where(pick, 1.0, 0.0).astype(BF16)

        def choose(b, d=d, pick=pick):
            place = lax.broadcasted_iota(jnp.int32, (block, group), 0) + b * block
            chosen = jnp.where(place == relayout_ref[d : d + 1, :], 1.0, 0.0).astype(BF16)
            select[d, b] = contract(pick, chosen, 1).astype(BF16)

        each(blocks, choose)
        column = lax.broadcasted_iota(jnp.int32, (wide, rows), 0)
        row = lax.broadcasted_iota(jnp.int32, (wide, rows), 1)
        table = jnp.where(column == row + HALO, 1.0, 0.0)
        for k in range(LINK_COUNT):
            link = near_ref[LINK_COUNT * d + k : LINK_COUNT * d + k + 1, :] - (me * rows - HALO)
            table = table - jnp.where(column == link, 1.0 / LINK_COUNT, 0.0)
        own_links[d] = table.T.astype(BF16)

    duals[...] = jnp.zeros_like(duals)
    duals[:, :horizon] = capacity_ref[...]
    capacity = duals[...]
    flow[...] = jnp.zeros_like(flow)
    links[...] = jnp.full_like(links, -window * 4)

    near[me] = near_ref[...]
    owned[me] = owner_ref[...]
    for step in range(1, sub_count):
        source = lax.rem(me + step, sub_count)
        for source_ref, place_ref, send_sem, recv_sem in (
            (near_ref, near, near_send, near_recv),
            (owner_ref, owned, owner_send, owner_recv),
        ):
            pltpu.make_async_remote_copy(
                src_ref=source_ref,
                dst_ref=place_ref.at[source],
                send_sem=send_sem.at[step],
                recv_sem=recv_sem.at[source],
                device_id={"sub": source},
                device_id_type=MESH,
            ).wait_recv()
    for source in range(sub_count):
        links[:, HALO + source * rows : HALO + (source + 1) * rows] = near[source]
        owners[:, source * rows : (source + 1) * rows] = owned[source]
    for d in range(districts):
        own = owners[d : d + 1, :]
        hit = jnp.where(
            lax.broadcasted_iota(jnp.int32, (RESERVOIRS, group), 0) == own, 1.0, 0.0
        ).astype(F32)
        match_t[d] = hit.astype(BF16)
        match[d] = hit.T.astype(BF16)

        def build(b, d=d):
            start = b * block if isinstance(b, int) else pl.multiple_of(b * block, block)
            column = lax.broadcasted_iota(jnp.int32, (window, window), 0)
            row = lax.broadcasted_iota(jnp.int32, (window, window), 1)
            table = jnp.where(column == row, 1.0, 0.0)
            for k in range(LINK_COUNT):
                at = LINK_COUNT * d + k
                link = links[at : at + 1, pl.ds(start, window)] - (start - HALO)
                table = table - jnp.where(column == link, 1.0 / LINK_COUNT, 0.0)
            table = table.T.astype(BF16)
            spread[d, b] = mm(table[HALO : HALO + block], table).astype(BF16)

        each(blocks, build)

    for step in range(1, sub_count):
        source = lax.rem(me + step, sub_count)
        pltpu.make_async_remote_copy(
            src_ref=gathered.at[:, mine, :],
            dst_ref=gathered.at[:, pl.ds(pl.multiple_of(source * rows, rows), rows), :],
            send_sem=flow_send.at[step],
            recv_sem=flow_recv.at[source],
            device_id={"sub": source},
            device_id_type=MESH,
        ).wait_recv()

    def at_block(b, extra=0, size=block):
        return pl.ds(b * block + extra, size)

    for d in range(districts):
        def permute(b, d=d):
            place = lax.broadcasted_iota(jnp.int32, (block, group), 0) + b * block
            chosen = jnp.where(place == relayout_ref[d : d + 1, :], 1.0, 0.0).astype(BF16)
            moved = mm(chosen, gathered[d])
            base[d, at_block(b), :] = moved
            flow[d, at_block(b, HALO), :] = moved.astype(BF16)

        each(blocks, permute)

    own_window = pl.ds(pl.multiple_of(me * rows, rows), wide)
    for d in range(districts):
        total[d] = flow[d, own_window, :].astype(F32)

        def begin(b, d=d):
            state[d, at_block(b), :] = price_step * mm(spread[d, b], flow[d, at_block(b, 0, window), :])

        each(blocks, begin)

    def forward():
        for d in range(districts):
            def one(b, d=d):
                price = state[d, at_block(b), :].astype(BF16)
                flow[d, at_block(b, HALO), :] = (base[d, at_block(b), :] + mm(price, weight[d])).astype(BF16)

            each(blocks, one)
            total[d] += flow[d, own_window, :].astype(F32)

    def backward():
        for d in range(districts):
            def one(b, d=d):
                state[d, at_block(b), :] += price_step * mm(
                    spread[d, b], flow[d, at_block(b, 0, window), :]
                )

            each(blocks, one)

    def inner(step, carry):
        forward()
        backward()
        return carry

    def send_draws(outer):
        drawn = mm(match_t[0], flow[0, HALO : HALO + group, :])
        for d in range(1, districts):
            drawn = drawn + mm(match_t[d], flow[d, HALO : HALO + group, :])
        draws[outer] = drawn[:, :LANES]
        copies = []
        for step in range(1, district_count):
            copies.append(
                pltpu.make_async_remote_copy(
                    src_ref=draws.at[outer],
                    dst_ref=arrived.at[outer, step],
                    send_sem=draw_send.at[outer, step],
                    recv_sem=draw_recv.at[outer, step],
                    device_id={"district": lax.rem(my_district + step, district_count)},
                    device_id_type=MESH,
                )
            )
            copies[-1].start()
        return copies

    def take_draws(outer, copies):
        drawn = draws[outer]
        for step in range(1, district_count):
            copies[step - 1].wait()
            drawn = drawn + arrived[outer, step]
        lane = lax.broadcasted_iota(jnp.int32, drawn.shape, 1)
        return jnp.where(lane < horizon, (drawn - capacity) * dual_scale, 0.0)

    lax.fori_loop(1, INNER_ITERS - 1, inner, 0)
    forward()
    copies = send_draws(0)
    backward()
    moved = take_draws(0, copies)
    for outer in range(1, OUTER_ITERS):
        duals[...] = moved if outer == 1 else duals[...] + moved
        high = moved.astype(BF16)
        low = (moved - high.astype(F32)).astype(BF16)
        for d in range(districts):
            state[d, :, :LANES] += mm(match[d], high) + mm(match[d], low)
        lax.fori_loop(0, INNER_ITERS - 1, inner, 0)
        forward()
        copies = send_draws(outer)
        if outer < OUTER_ITERS - 1:
            backward()
        else:
            for d in range(districts):
                price = state[d].astype(BF16)
                chosen = mm(select[d, 0], price[:block])
                for b in range(1, blocks):
                    chosen = chosen + mm(select[d, b], price[b * block : (b + 1) * block])
                chosen = chosen.astype(BF16)
                gradient = costs_ref[d].astype(F32) + mm(chosen, coupling[d])
                plan_ref[d] = -mm(gradient.astype(BF16), factor[d])
                summed = total[d]
                high = summed.astype(BF16)
                low = (summed - high.astype(F32)).astype(BF16)
                prices_ref[d] = price_step * (mm(own_links[d], high) + mm(own_links[d], low))
        moved = take_draws(outer, copies)
    duals_ref[...] = (duals[...] + moved)[:, :horizon]
    for send in sends:
        send.wait_send()


def handover(plan_ref, prices_ref, duals_ref, plan_out, prices_out, duals_out, sem):
    copies = [
        pltpu.make_async_copy(source, target, sem.at[index])
        for index, (source, target) in enumerate(
            ((plan_ref, plan_out), (prices_ref, prices_out), (duals_ref, duals_out))
        )
    ]
    for copy in copies:
        copy.start()
    for copy in copies:
        copy.wait()


def on_device(cost_terms, neighbours, relayout, ownership, capacity, coupling, solve_factor):
    districts, rows, unknowns = cost_terms.shape
    interface = coupling.shape[2]
    group = relayout.shape[1]
    sub_count = lax.axis_size("sub")
    district_count = lax.axis_size("district")
    load_count = districts * district_count * group // (2 * RESERVOIRS)
    dual_scale = reserve_step / math.sqrt(load_count)
    near = neighbours.transpose(0, 2, 1).reshape(districts * LINK_COUNT, rows)
    coupling = coupling.transpose(0, 2, 1)
    block = 2 * rows
    blocks = group // block
    window = block + 2 * HALO
    vmem = pl.BlockSpec(memory_space=pltpu.VMEM)
    hbm = pl.BlockSpec(memory_space=pl.ANY)
    dma = pltpu.SemaphoreType.DMA
    results = pl.pallas_call(
        functools.partial(kernel, dual_scale),
        name="districts",
        out_shape=(
            jax.ShapeDtypeStruct((districts, rows, unknowns), F32),
            jax.ShapeDtypeStruct((districts, rows, interface), F32),
            jax.ShapeDtypeStruct(capacity.shape, F32),
        ),
        in_specs=[vmem, vmem, vmem, vmem, vmem, hbm, hbm],
        out_specs=(vmem, vmem, vmem),
        scratch_shapes=[
            pltpu.VMEM(coupling.shape, BF16),
            pltpu.VMEM(solve_factor.shape, BF16),
            pltpu.VMEM((sub_count,) + near.shape, jnp.int32),
            pltpu.VMEM((sub_count,) + ownership.shape, jnp.int32),
            pltpu.VMEM((districts * LINK_COUNT, group + 2 * HALO), jnp.int32),
            pltpu.VMEM((districts, group), jnp.int32),
            pltpu.VMEM((districts, group, interface), BF16),
            pltpu.VMEM((districts, group, interface), F32),
            pltpu.VMEM((districts, group, interface), F32),
            pltpu.VMEM((districts, group + 2 * HALO, interface), BF16),
            pltpu.VMEM((districts, rows + 2 * HALO, interface), F32),
            pltpu.VMEM((districts, blocks, block, window), BF16),
            pltpu.VMEM((districts, interface, interface), BF16),
            pltpu.VMEM((districts, group, RESERVOIRS), BF16),
            pltpu.VMEM((districts, RESERVOIRS, group), BF16),
            pltpu.VMEM((districts, blocks, rows, block), BF16),
            pltpu.VMEM((districts, rows, rows + 2 * HALO), BF16),
            pltpu.VMEM((RESERVOIRS, LANES), F32),
            pltpu.VMEM((OUTER_ITERS, RESERVOIRS, LANES), F32),
            pltpu.VMEM((OUTER_ITERS, district_count, RESERVOIRS, LANES), F32),
            dma((2 * districts,)),
            dma((sub_count,)),
            dma((sub_count,)),
            dma((sub_count,)),
            dma((sub_count,)),
            dma((sub_count,)),
            dma((sub_count,)),
            dma((OUTER_ITERS, district_count)),
            dma((OUTER_ITERS, district_count)),
        ],
        compiler_params=pltpu.CompilerParams(
            collective_id=0, has_side_effects=True, vmem_limit_bytes=(20 if group <= 1024 else 60) * 1024 * 1024
        ),
    )(cost_terms, near, ownership, relayout, capacity, coupling, solve_factor)
    return pl.pallas_call(
        handover,
        name="handover",
        out_shape=tuple(jax.ShapeDtypeStruct(value.shape, value.dtype) for value in results),
        in_specs=[hbm] * 3,
        out_specs=(hbm,) * 3,
        scratch_shapes=[dma((3,))],
        compiler_params=pltpu.CompilerParams(vmem_limit_bytes=4 * 1024 * 1024),
    )(*results)


def solution(mesh):
    placed = (
        P("district", "sub", None),
        P("district", "sub", None),
        P("district", None),
        P("district", "sub"),
        P(),
        P("district", None, None),
        P("district", None, None),
    )
    return jax.shard_map(
        on_device,
        mesh=mesh,
        in_specs=placed,
        out_specs=(P("district", "sub", None), P("district", "sub", None), P()),
        check_vma=False,
    )
```

```python
import functools
import math

import jax
import jax.numpy as jnp
from jax import lax
from jax.experimental import pallas as pl
from jax.experimental.pallas import tpu as pltpu
from jax.sharding import PartitionSpec as P

REACH_SPAN = 16
LINK_COUNT = 4
RESERVOIRS = 16
OUTER_ITERS = 2
INNER_ITERS = 4
HALO = 2 * REACH_SPAN
LANES = 128

price_step = 0.3
reserve_step = 1.0

F32 = jnp.float32
BF16 = jnp.bfloat16
MESH = pl.DeviceIdType.MESH


def each(count, body):
    if count <= 8:
        for index in range(count):
            body(index)
    else:
        lax.fori_loop(0, count, lambda index, carry: (body(index), carry)[1], 0)


def mm(a, b):
    return jnp.dot(a, b, preferred_element_type=F32)


def contract(a, b, dim):
    return lax.dot_general(a, b, (((dim,), (dim,)), ((), ())), preferred_element_type=F32)


def kernel(
    dual_scale, costs_hbm, near_hbm, owner_hbm, relayout_hbm, capacity_hbm, coupling_hbm, factor_hbm,
    plan_ref, prices_ref, duals_ref,
    costs_ref, near_ref, owner_ref, relayout_ref, capacity_ref, coupling, factor, near, owned, links, owners, gathered, base, state, flow, total, spread, weight,
    match, match_t, select, own_links, duals, draws, arrived,
    local_sem, near_send, near_recv, owner_send, owner_recv, flow_send, flow_recv, draw_send, draw_recv,
):
    districts, rows, unknowns = costs_ref.shape
    interface = coupling.shape[1]
    horizon = capacity_ref.shape[1]
    group = relayout_ref.shape[1]
    sub_count = lax.axis_size("sub")
    district_count = lax.axis_size("district")
    me = lax.axis_index("sub")
    my_district = lax.axis_index("district")
    block = 2 * rows
    window = block + 2 * HALO
    blocks = group // block

    costs_load = pltpu.make_async_copy(costs_hbm, costs_ref, local_sem.at[2 * districts])
    costs_load.start()
    loads = []
    for d in range(districts):
        loads.append(
            (
                pltpu.make_async_copy(factor_hbm.at[d], factor.at[d], local_sem.at[2 * d]),
                pltpu.make_async_copy(coupling_hbm.at[d], coupling.at[d], local_sem.at[2 * d + 1]),
            )
        )
        for load in loads[-1]:
            load.start()

    small_loads = [
        pltpu.make_async_copy(source, target, local_sem.at[2 * districts + 1 + index])
        for index, (source, target) in enumerate(
            (
                (near_hbm, near_ref),
                (owner_hbm, owner_ref),
                (relayout_hbm, relayout_ref),
                (capacity_hbm, capacity_ref),
            )
        )
    ]
    for load in small_loads:
        load.start()

    barrier = pltpu.get_barrier_semaphore()
    for step in range(1, sub_count):
        pl.semaphore_signal(
            barrier, inc=1, device_id={"sub": lax.rem(me + step, sub_count)}, device_id_type=MESH
        )
    for step in range(1, district_count):
        pl.semaphore_signal(
            barrier,
            inc=1,
            device_id={"district": lax.rem(my_district + step, district_count)},
            device_id_type=MESH,
        )

    costs_load.wait()
    mine = pl.ds(pl.multiple_of(me * rows, rows), rows)
    for d in range(districts):
        for load in loads[d]:
            load.wait()
        first_plan = -mm(costs_ref[d], factor[d])
        gathered[d, mine, :] = contract(first_plan.astype(BF16), coupling[d], 1).astype(BF16)

    for load in small_loads:
        load.wait()
    pl.semaphore_wait(barrier, sub_count - 1 + district_count - 1)
    sends = []
    for step in range(1, sub_count):
        target = lax.rem(me + step, sub_count)
        for source_ref, place_ref, send_sem, recv_sem in (
            (near_ref, near, near_send, near_recv),
            (owner_ref, owned, owner_send, owner_recv),
        ):
            sends.append(
                pltpu.make_async_remote_copy(
                    src_ref=source_ref,
                    dst_ref=place_ref.at[me],
                    send_sem=send_sem.at[step],
                    recv_sem=recv_sem.at[me],
                    device_id={"sub": target},
                    device_id_type=MESH,
                )
            )
            sends[-1].start()
    for step in range(1, sub_count):
        target = lax.rem(me + step, sub_count)
        sends.append(
            pltpu.make_async_remote_copy(
                src_ref=gathered.at[:, mine, :],
                dst_ref=gathered.at[:, mine, :],
                send_sem=flow_send.at[step],
                recv_sem=flow_recv.at[me],
                device_id={"sub": target},
                device_id_type=MESH,
            )
        )
        sends[-1].start()

    for d in range(districts):
        narrow = mm(coupling[d], factor[d]).astype(BF16)
        weight[d] = (-contract(narrow, coupling[d], 1)).astype(BF16)

    wide = rows + 2 * HALO
    for d in range(districts):
        pick = lax.broadcasted_iota(jnp.int32, (rows, group), 1) == (
            lax.broadcasted_iota(jnp.int32, (rows, group), 0) + me * rows
        )
        pick = jnp.where(pick, 1.0, 0.0).astype(BF16)

        def choose(b, d=d, pick=pick):
            place = lax.broadcasted_iota(jnp.int32, (block, group), 0) + b * block
            chosen = jnp.where(place == relayout_ref[d : d + 1, :], 1.0, 0.0).astype(BF16)
            select[d, b] = contract(pick, chosen, 1).astype(BF16)

        each(blocks, choose)
        column = lax.broadcasted_iota(jnp.int32, (wide, rows), 0)
        row = lax.broadcasted_iota(jnp.int32, (wide, rows), 1)
        table = jnp.where(column == row + HALO, 1.0, 0.0)
        for k in range(LINK_COUNT):
            link = near_ref[LINK_COUNT * d + k : LINK_COUNT * d + k + 1, :] - (me * rows - HALO)
            table = table - jnp.where(column == link, 1.0 / LINK_COUNT, 0.0)
        own_links[d] = table.T.astype(BF16)

    duals[...] = jnp.zeros_like(duals)
    duals[:, :horizon] = capacity_ref[...]
    capacity = duals[...]
    flow[...] = jnp.zeros_like(flow)
    links[...] = jnp.full_like(links, -window * 4)

    near[me] = near_ref[...]
    owned[me] = owner_ref[...]
    for step in range(1, sub_count):
        source = lax.rem(me + step, sub_count)
        for source_ref, place_ref, send_sem, recv_sem in (
            (near_ref, near, near_send, near_recv),
            (owner_ref, owned, owner_send, owner_recv),
        ):
            pltpu.make_async_remote_copy(
                src_ref=source_ref,
                dst_ref=place_ref.at[source],
                send_sem=send_sem.at[step],
                recv_sem=recv_sem.at[source],
                device_id={"sub": source},
                device_id_type=MESH,
            ).wait_recv()
    for source in range(sub_count):
        links[:, HALO + source * rows : HALO + (source + 1) * rows] = near[source]
        owners[:, source * rows : (source + 1) * rows] = owned[source]
    for d in range(districts):
        own = owners[d : d + 1, :]
        hit = jnp.where(
            lax.broadcasted_iota(jnp.int32, (RESERVOIRS, group), 0) == own, 1.0, 0.0
        ).astype(F32)
        match_t[d] = hit.astype(BF16)
        match[d] = hit.T.astype(BF16)

        def build(b, d=d):
            start = b * block if isinstance(b, int) else pl.multiple_of(b * block, block)
            column = lax.broadcasted_iota(jnp.int32, (window, window), 0)
            row = lax.broadcasted_iota(jnp.int32, (window, window), 1)
            table = jnp.where(column == row, 1.0, 0.0)
            for k in range(LINK_COUNT):
                at = LINK_COUNT * d + k
                link = links[at : at + 1, pl.ds(start, window)] - (start - HALO)
                table = table - jnp.where(column == link, 1.0 / LINK_COUNT, 0.0)
            table = table.T.astype(BF16)
            spread[d, b] = mm(table[HALO : HALO + block], table).astype(BF16)

        each(blocks, build)

    for step in range(1, sub_count):
        source = lax.rem(me + step, sub_count)
        pltpu.make_async_remote_copy(
            src_ref=gathered.at[:, mine, :],
            dst_ref=gathered.at[:, pl.ds(pl.multiple_of(source * rows, rows), rows), :],
            send_sem=flow_send.at[step],
            recv_sem=flow_recv.at[source],
            device_id={"sub": source},
            device_id_type=MESH,
        ).wait_recv()

    def at_block(b, extra=0, size=block):
        return pl.ds(b * block + extra, size)

    for d in range(districts):
        def permute(b, d=d):
            place = lax.broadcasted_iota(jnp.int32, (block, group), 0) + b * block
            chosen = jnp.where(place == relayout_ref[d : d + 1, :], 1.0, 0.0).astype(BF16)
            moved = mm(chosen, gathered[d])
            base[d, at_block(b), :] = moved
            flow[d, at_block(b, HALO), :] = moved.astype(BF16)

        each(blocks, permute)

    own_window = pl.ds(pl.multiple_of(me * rows, rows), wide)
    for d in range(districts):
        total[d] = flow[d, own_window, :].astype(F32)

        def begin(b, d=d):
            state[d, at_block(b), :] = price_step * mm(spread[d, b], flow[d, at_block(b, 0, window), :])

        each(blocks, begin)

    def forward():
        for d in range(districts):
            def one(b, d=d):
                price = state[d, at_block(b), :].astype(BF16)
                flow[d, at_block(b, HALO), :] = (base[d, at_block(b), :] + mm(price, weight[d])).astype(BF16)

            each(blocks, one)
            total[d] += flow[d, own_window, :].astype(F32)

    def backward():
        for d in range(districts):
            def one(b, d=d):
                state[d, at_block(b), :] += price_step * mm(
                    spread[d, b], flow[d, at_block(b, 0, window), :]
                )

            each(blocks, one)

    def inner(step, carry):
        forward()
        backward()
        return carry

    def send_draws(outer):
        drawn = mm(match_t[0], flow[0, HALO : HALO + group, :])
        for d in range(1, districts):
            drawn = drawn + mm(match_t[d], flow[d, HALO : HALO + group, :])
        draws[outer] = drawn[:, :LANES]
        copies = []
        for step in range(1, district_count):
            copies.append(
                pltpu.make_async_remote_copy(
                    src_ref=draws.at[outer],
                    dst_ref=arrived.at[outer, step],
                    send_sem=draw_send.at[outer, step],
                    recv_sem=draw_recv.at[outer, step],
                    device_id={"district": lax.rem(my_district + step, district_count)},
                    device_id_type=MESH,
                )
            )
            copies[-1].start()
        return copies

    def take_draws(outer, copies):
        drawn = draws[outer]
        for step in range(1, district_count):
            copies[step - 1].wait()
            drawn = drawn + arrived[outer, step]
        lane = lax.broadcasted_iota(jnp.int32, drawn.shape, 1)
        return jnp.where(lane < horizon, (drawn - capacity) * dual_scale, 0.0)

    lax.fori_loop(1, INNER_ITERS - 1, inner, 0)
    forward()
    copies = send_draws(0)
    backward()
    moved = take_draws(0, copies)
    for outer in range(1, OUTER_ITERS):
        duals[...] = moved if outer == 1 else duals[...] + moved
        high = moved.astype(BF16)
        low = (moved - high.astype(F32)).astype(BF16)
        for d in range(districts):
            state[d, :, :LANES] += mm(match[d], high) + mm(match[d], low)
        lax.fori_loop(0, INNER_ITERS - 1, inner, 0)
        forward()
        copies = send_draws(outer)
        if outer < OUTER_ITERS - 1:
            backward()
        else:
            for d in range(districts):
                price = state[d].astype(BF16)
                chosen = mm(select[d, 0], price[:block])
                for b in range(1, blocks):
                    chosen = chosen + mm(select[d, b], price[b * block : (b + 1) * block])
                chosen = chosen.astype(BF16)
                gradient = costs_ref[d].astype(F32) + mm(chosen, coupling[d])
                plan_ref[d] = -mm(gradient.astype(BF16), factor[d])
                summed = total[d]
                high = summed.astype(BF16)
                low = (summed - high.astype(F32)).astype(BF16)
                prices_ref[d] = price_step * (mm(own_links[d], high) + mm(own_links[d], low))
        moved = take_draws(outer, copies)
    duals_ref[...] = (duals[...] + moved)[:, :horizon]
    for send in sends:
        send.wait_send()


def handover(plan_ref, prices_ref, duals_ref, plan_out, prices_out, duals_out, sem):
    copies = [
        pltpu.make_async_copy(source, target, sem.at[index])
        for index, (source, target) in enumerate(
            ((plan_ref, plan_out), (prices_ref, prices_out), (duals_ref, duals_out))
        )
    ]
    for copy in copies:
        copy.start()
    for copy in copies:
        copy.wait()


def on_device(cost_terms, neighbours, relayout, ownership, capacity, coupling, solve_factor):
    districts, rows, unknowns = cost_terms.shape
    interface = coupling.shape[2]
    group = relayout.shape[1]
    sub_count = lax.axis_size("sub")
    district_count = lax.axis_size("district")
    load_count = districts * district_count * group // (2 * RESERVOIRS)
    dual_scale = reserve_step / math.sqrt(load_count)
    near = neighbours.transpose(0, 2, 1).reshape(districts * LINK_COUNT, rows)
    coupling = coupling.transpose(0, 2, 1)
    block = 2 * rows
    blocks = group // block
    window = block + 2 * HALO
    vmem = pl.BlockSpec(memory_space=pltpu.VMEM)
    hbm = pl.BlockSpec(memory_space=pl.ANY)
    dma = pltpu.SemaphoreType.DMA
    results = pl.pallas_call(
        functools.partial(kernel, dual_scale),
        name="districts",
        out_shape=(
            jax.ShapeDtypeStruct((districts, rows, unknowns), F32),
            jax.ShapeDtypeStruct((districts, rows, interface), F32),
            jax.ShapeDtypeStruct(capacity.shape, F32),
        ),
        in_specs=[pl.BlockSpec(memory_space=pltpu.HBM)] * 7,
        out_specs=(vmem, vmem, vmem),
        scratch_shapes=[
            pltpu.VMEM(cost_terms.shape, BF16),
            pltpu.VMEM(near.shape, jnp.int32),
            pltpu.VMEM(ownership.shape, jnp.int32),
            pltpu.VMEM(relayout.shape, jnp.int32),
            pltpu.VMEM(capacity.shape, F32),
            pltpu.VMEM(coupling.shape, BF16),
            pltpu.VMEM(solve_factor.shape, BF16),
            pltpu.VMEM((sub_count,) + near.shape, jnp.int32),
            pltpu.VMEM((sub_count,) + ownership.shape, jnp.int32),
            pltpu.VMEM((districts * LINK_COUNT, group + 2 * HALO), jnp.int32),
            pltpu.VMEM((districts, group), jnp.int32),
            pltpu.VMEM((districts, group, interface), BF16),
            pltpu.VMEM((districts, group, interface), F32),
            pltpu.VMEM((districts, group, interface), F32),
            pltpu.VMEM((districts, group + 2 * HALO, interface), BF16),
            pltpu.VMEM((districts, rows + 2 * HALO, interface), F32),
            pltpu.VMEM((districts, blocks, block, window), BF16),
            pltpu.VMEM((districts, interface, interface), BF16),
            pltpu.VMEM((districts, group, RESERVOIRS), BF16),
            pltpu.VMEM((districts, RESERVOIRS, group), BF16),
            pltpu.VMEM((districts, blocks, rows, block), BF16),
            pltpu.VMEM((districts, rows, rows + 2 * HALO), BF16),
            pltpu.VMEM((RESERVOIRS, LANES), F32),
            pltpu.VMEM((OUTER_ITERS, RESERVOIRS, LANES), F32),
            pltpu.VMEM((OUTER_ITERS, district_count, RESERVOIRS, LANES), F32),
            dma((2 * districts + 5,)),
            dma((sub_count,)),
            dma((sub_count,)),
            dma((sub_count,)),
            dma((sub_count,)),
            dma((sub_count,)),
            dma((sub_count,)),
            dma((OUTER_ITERS, district_count)),
            dma((OUTER_ITERS, district_count)),
        ],
        compiler_params=pltpu.CompilerParams(
            collective_id=0, has_side_effects=True, vmem_limit_bytes=(20 if group <= 1024 else 60) * 1024 * 1024
        ),
    )(*[pltpu.with_memory_space_constraint(value, pltpu.HBM) for value in (cost_terms, near, ownership, relayout, capacity, coupling, solve_factor)])
    return pl.pallas_call(
        handover,
        name="handover",
        out_shape=tuple(jax.ShapeDtypeStruct(value.shape, value.dtype) for value in results),
        in_specs=[hbm] * 3,
        out_specs=(hbm,) * 3,
        scratch_shapes=[dma((3,))],
        compiler_params=pltpu.CompilerParams(vmem_limit_bytes=4 * 1024 * 1024),
    )(*results)


def solution(mesh):
    placed = (
        P("district", "sub", None),
        P("district", "sub", None),
        P("district", None),
        P("district", "sub"),
        P(),
        P("district", None, None),
        P("district", None, None),
    )
    return jax.shard_map(
        on_device,
        mesh=mesh,
        in_specs=placed,
        out_specs=(P("district", "sub", None), P("district", "sub", None), P()),
        check_vma=False,
    )
```

```python
import functools
import math

import jax
import jax.numpy as jnp
from jax import lax
from jax.experimental import pallas as pl
from jax.experimental.pallas import tpu as pltpu
from jax.sharding import PartitionSpec as P

REACH_SPAN = 16
LINK_COUNT = 4
RESERVOIRS = 16
OUTER_ITERS = 2
INNER_ITERS = 4
HALO = 2 * REACH_SPAN
LANES = 128

price_step = 0.3
reserve_step = 1.0

F32 = jnp.float32
BF16 = jnp.bfloat16
MESH = pl.DeviceIdType.MESH


def each(count, body):
    if count <= 8:
        for index in range(count):
            body(index)
    else:
        lax.fori_loop(0, count, lambda index, carry: (body(index), carry)[1], 0)


def mm(a, b):
    return jnp.dot(a, b, preferred_element_type=F32)


def contract(a, b, dim):
    return lax.dot_general(a, b, (((dim,), (dim,)), ((), ())), preferred_element_type=F32)


def kernel(
    dual_scale, costs_hbm, near_hbm, owner_hbm, relayout_hbm, capacity_hbm, coupling_hbm, factor_hbm,
    plan_ref, prices_ref, duals_ref,
    costs_ref, near_ref, owner_ref, relayout_ref, capacity_ref, coupling, factor, near, owned, links, owners, first, gathered, base, state, flow, total, spread, weight,
    match, match_t, select, near_links, chosen_out, chosen_in, prices_out, prices_in, duals, draws, arrived,
    local_sem, near_send, near_recv, owner_send, owner_recv, flow_send, flow_recv, draw_send, draw_recv,
    price_send, price_recv, dual_send, dual_recv,
):
    districts, rows, unknowns = costs_ref.shape
    interface = coupling.shape[1]
    horizon = capacity_ref.shape[1]
    group = relayout_ref.shape[1]
    sub_count = lax.axis_size("sub")
    district_count = lax.axis_size("district")
    me = lax.axis_index("sub")
    role = lax.rem(me, districts)
    team = me // districts * districts
    my_district = lax.axis_index("district")
    block = districts * rows
    window = block + 2 * HALO
    blocks = group // block

    costs_load = pltpu.make_async_copy(costs_hbm, costs_ref, local_sem.at[2 * districts])
    costs_load.start()
    loads = []
    for d in range(districts):
        loads.append(
            (
                pltpu.make_async_copy(factor_hbm.at[d], factor.at[d], local_sem.at[2 * d]),
                pltpu.make_async_copy(coupling_hbm.at[d], coupling.at[d], local_sem.at[2 * d + 1]),
            )
        )
        for load in loads[-1]:
            load.start()

    small_loads = [
        pltpu.make_async_copy(source, target, local_sem.at[2 * districts + 1 + index])
        for index, (source, target) in enumerate(
            (
                (near_hbm, near_ref),
                (owner_hbm, owner_ref),
                (relayout_hbm, relayout_ref),
                (capacity_hbm, capacity_ref),
            )
        )
    ]
    for load in small_loads:
        load.start()

    barrier = pltpu.get_barrier_semaphore()
    for step in range(1, sub_count):
        pl.semaphore_signal(
            barrier, inc=1, device_id={"sub": lax.rem(me + step, sub_count)}, device_id_type=MESH
        )
    for step in range(1, district_count):
        for other in range(districts):
            pl.semaphore_signal(
                barrier,
                inc=1,
                device_id={
                    "district": lax.rem(my_district + step, district_count),
                    "sub": team + lax.rem(role + other, districts),
                },
                device_id_type=MESH,
            )

    costs_load.wait()
    mine = pl.ds(pl.multiple_of(me * rows, rows), rows)
    for d in range(districts):
        for load in loads[d]:
            load.wait()
        first_plan = -mm(costs_ref[d], factor[d])
        first[d] = contract(first_plan.astype(BF16), coupling[d], 1).astype(BF16)

    for load in small_loads:
        load.wait()
    pl.semaphore_wait(barrier, sub_count - 1 + (district_count - 1) * districts)
    sends = []
    for step in range(1, sub_count):
        target = lax.rem(me + step, sub_count)
        for source_ref, place_ref, send_sem, recv_sem in (
            (near_ref, near, near_send, near_recv),
            (owner_ref, owned, owner_send, owner_recv),
        ):
            sends.append(
                pltpu.make_async_remote_copy(
                    src_ref=source_ref,
                    dst_ref=place_ref.at[me],
                    send_sem=send_sem.at[step],
                    recv_sem=recv_sem.at[me],
                    device_id={"sub": target},
                    device_id_type=MESH,
                )
            )
            sends[-1].start()
    for step in range(1, sub_count):
        target = lax.rem(me + step, sub_count)
        sends.append(
            pltpu.make_async_remote_copy(
                src_ref=first.at[lax.rem(target, districts)],
                dst_ref=gathered.at[mine, :],
                send_sem=flow_send.at[step],
                recv_sem=flow_recv.at[me],
                device_id={"sub": target},
                device_id_type=MESH,
            )
        )
        sends[-1].start()

    gathered[mine, :] = first[role]
    narrow = mm(coupling[role], factor[role]).astype(BF16)
    weight[...] = (-contract(narrow, coupling[role], 1)).astype(BF16)

    wide = rows + 2 * HALO
    moves = relayout_ref[pl.ds(role, 1), :]
    team_rows = districts * rows
    pick = lax.broadcasted_iota(jnp.int32, (team_rows, group), 1) == (
        lax.broadcasted_iota(jnp.int32, (team_rows, group), 0) + team * rows
    )
    pick = jnp.where(pick, 1.0, 0.0).astype(BF16)

    def choose(b):
        place = lax.broadcasted_iota(jnp.int32, (block, group), 0) + b * block
        chosen = jnp.where(place == moves, 1.0, 0.0).astype(BF16)
        select[b] = contract(pick, chosen, 1).astype(BF16)

    each(blocks, choose)

    duals[...] = jnp.zeros_like(duals)
    duals[:, :horizon] = capacity_ref[...]
    capacity = duals[...]
    flow[...] = jnp.zeros_like(flow)
    links[...] = jnp.full_like(links, -window * 4)

    near[me] = near_ref[...]
    owned[me] = owner_ref[...]
    for step in range(1, sub_count):
        source = lax.rem(me + step, sub_count)
        for source_ref, place_ref, send_sem, recv_sem in (
            (near_ref, near, near_send, near_recv),
            (owner_ref, owned, owner_send, owner_recv),
        ):
            pltpu.make_async_remote_copy(
                src_ref=source_ref,
                dst_ref=place_ref.at[source],
                send_sem=send_sem.at[step],
                recv_sem=recv_sem.at[source],
                device_id={"sub": source},
                device_id_type=MESH,
            ).wait_recv()
    for source in range(sub_count):
        links[:, HALO + source * rows : HALO + (source + 1) * rows] = near[source]
        owners[:, source * rows : (source + 1) * rows] = owned[source]
    own = owners[pl.ds(role, 1), :]
    hit = jnp.where(
        lax.broadcasted_iota(jnp.int32, (RESERVOIRS, group), 0) == own, 1.0, 0.0
    ).astype(F32)
    match_t[...] = hit.astype(BF16)
    match[...] = hit.T.astype(BF16)

    def linked(start, width):
        column = lax.broadcasted_iota(jnp.int32, (width, width), 0)
        row = lax.broadcasted_iota(jnp.int32, (width, width), 1)
        table = jnp.where(column == row, 1.0, 0.0)
        for k in range(LINK_COUNT):
            link = links[pl.ds(role * LINK_COUNT + k, 1), pl.ds(start, width)] - (start - HALO)
            table = table - jnp.where(column == link, 1.0 / LINK_COUNT, 0.0)
        return table.T.astype(BF16)

    def build(b):
        start = b * block if isinstance(b, int) else pl.multiple_of(b * block, block)
        table = linked(start, window)
        spread[b] = mm(table[HALO : HALO + block], table).astype(BF16)

    each(blocks, build)
    near_links[...] = linked(pl.multiple_of(team * rows, team_rows), window)[HALO : HALO + team_rows]

    for step in range(1, sub_count):
        source = lax.rem(me + step, sub_count)
        pltpu.make_async_remote_copy(
            src_ref=first.at[role],
            dst_ref=gathered.at[pl.ds(pl.multiple_of(source * rows, rows), rows), :],
            send_sem=flow_send.at[step],
            recv_sem=flow_recv.at[source],
            device_id={"sub": source},
            device_id_type=MESH,
        ).wait_recv()

    def at_block(b, extra=0, size=block):
        return pl.ds(b * block + extra, size)

    def permute(b):
        place = lax.broadcasted_iota(jnp.int32, (block, group), 0) + b * block
        chosen = jnp.where(place == moves, 1.0, 0.0).astype(BF16)
        moved = mm(chosen, gathered[...])
        base[at_block(b), :] = moved
        flow[at_block(b, HALO), :] = moved.astype(BF16)

    each(blocks, permute)

    team_window = pl.ds(pl.multiple_of(team * rows, team_rows), window)
    total[...] = flow[team_window, :].astype(F32)

    def begin(b):
        state[at_block(b), :] = price_step * mm(spread[b], flow[at_block(b, 0, window), :])

    each(blocks, begin)

    def forward():
        def one(b):
            price = state[at_block(b), :].astype(BF16)
            flow[at_block(b, HALO), :] = (base[at_block(b), :] + mm(price, weight[...])).astype(BF16)

        each(blocks, one)
        total[...] += flow[team_window, :].astype(F32)

    def backward():
        def one(b):
            state[at_block(b), :] += price_step * mm(spread[b], flow[at_block(b, 0, window), :])

        each(blocks, one)

    def inner(step, carry):
        forward()
        backward()
        return carry

    partners = [
        (step, other)
        for step in range(district_count)
        for other in range(districts)
        if step or other
    ]

    def partner(step, other):
        return {
            "district": lax.rem(my_district + step, district_count),
            "sub": team + lax.rem(role + other, districts),
        }

    def send_draws(outer):
        drawn = mm(match_t[...], flow[HALO : HALO + group, :])
        draws[outer] = drawn[:, :LANES]
        copies = []
        for index, (step, other) in enumerate(partners):
            copies.append(
                pltpu.make_async_remote_copy(
                    src_ref=draws.at[outer],
                    dst_ref=arrived.at[outer, index],
                    send_sem=draw_send.at[outer, index],
                    recv_sem=draw_recv.at[outer, index],
                    device_id=partner(step, other),
                    device_id_type=MESH,
                )
            )
            copies[-1].start()
        return copies

    def take_draws(outer, copies):
        drawn = draws[outer]
        for index, copy in enumerate(copies):
            copy.wait()
            drawn = drawn + arrived[outer, index]
        lane = lax.broadcasted_iota(jnp.int32, drawn.shape, 1)
        return jnp.where(lane < horizon, (drawn - capacity) * dual_scale, 0.0)

    def to_team(source_ref, place_ref, send_sem, recv_sem):
        copies = []
        for other in range(1, districts):
            target = lax.rem(role + other, districts)
            copies.append(
                pltpu.make_async_remote_copy(
                    src_ref=source_ref.at[target],
                    dst_ref=place_ref.at[role],
                    send_sem=send_sem.at[other],
                    recv_sem=recv_sem.at[other],
                    device_id={"sub": team + target},
                    device_id_type=MESH,
                )
            )
            copies[-1].start()
        return copies

    lax.fori_loop(1, INNER_ITERS - 1, inner, 0)
    forward()
    copies = send_draws(0)
    backward()
    moved = take_draws(0, copies)
    for outer in range(1, OUTER_ITERS):
        duals[...] = moved if outer == 1 else duals[...] + moved
        high = moved.astype(BF16)
        low = (moved - high.astype(F32)).astype(BF16)
        state[:, :LANES] += mm(match[...], high) + mm(match[...], low)
        lax.fori_loop(0, INNER_ITERS - 1, inner, 0)
        if outer == OUTER_ITERS - 1:
            price = state[...].astype(BF16)
            chosen = mm(select[0], price[:block])
            for b in range(1, blocks):
                chosen = chosen + mm(select[b], price[b * block : (b + 1) * block])
            chosen_out[...] = chosen.reshape(districts, rows, -1).astype(BF16)
            price_copies = to_team(chosen_out, chosen_in, price_send, price_recv)
            chosen_in[role] = chosen_out[role]
        forward()
        copies = send_draws(outer)
        if outer < OUTER_ITERS - 1:
            backward()
        else:
            high = total[...].astype(BF16)
            low = (total[...] - high.astype(F32)).astype(BF16)
            prices = price_step * (mm(near_links[...], high) + mm(near_links[...], low))
            prices_out[...] = prices.reshape(districts, rows, -1)
            dual_copies = to_team(prices_out, prices_in, dual_send, dual_recv)
            prices_in[role] = prices_out[role]
            for copy in price_copies:
                copy.wait()
            for d in range(districts):
                gradient = costs_ref[d].astype(F32) + mm(chosen_in[d], coupling[d])
                plan_ref[d] = -mm(gradient.astype(BF16), factor[d])
            for copy in dual_copies:
                copy.wait()
            prices_ref[...] = prices_in[...]
        moved = take_draws(outer, copies)
    duals_ref[...] = (duals[...] + moved)[:, :horizon]
    for send in sends:
        send.wait_send()


def handover(plan_ref, prices_ref, duals_ref, plan_out, prices_out, duals_out, sem):
    copies = [
        pltpu.make_async_copy(source, target, sem.at[index])
        for index, (source, target) in enumerate(
            ((plan_ref, plan_out), (prices_ref, prices_out), (duals_ref, duals_out))
        )
    ]
    for copy in copies:
        copy.start()
    for copy in copies:
        copy.wait()


def on_device(cost_terms, neighbours, relayout, ownership, capacity, coupling, solve_factor):
    districts, rows, unknowns = cost_terms.shape
    interface = coupling.shape[2]
    group = relayout.shape[1]
    sub_count = lax.axis_size("sub")
    district_count = lax.axis_size("district")
    load_count = districts * district_count * group // (2 * RESERVOIRS)
    dual_scale = reserve_step / math.sqrt(load_count)
    near = neighbours.transpose(0, 2, 1).reshape(districts * LINK_COUNT, rows)
    coupling = coupling.transpose(0, 2, 1)
    block = districts * rows
    blocks = group // block
    window = block + 2 * HALO
    vmem = pl.BlockSpec(memory_space=pltpu.VMEM)
    hbm = pl.BlockSpec(memory_space=pl.ANY)
    dma = pltpu.SemaphoreType.DMA
    results = pl.pallas_call(
        functools.partial(kernel, dual_scale),
        name="districts",
        out_shape=(
            jax.ShapeDtypeStruct((districts, rows, unknowns), F32),
            jax.ShapeDtypeStruct((districts, rows, interface), F32),
            jax.ShapeDtypeStruct(capacity.shape, F32),
        ),
        in_specs=[pl.BlockSpec(memory_space=pltpu.HBM)] * 7,
        out_specs=(vmem, vmem, vmem),
        scratch_shapes=[
            pltpu.VMEM(cost_terms.shape, BF16),
            pltpu.VMEM(near.shape, jnp.int32),
            pltpu.VMEM(ownership.shape, jnp.int32),
            pltpu.VMEM(relayout.shape, jnp.int32),
            pltpu.VMEM(capacity.shape, F32),
            pltpu.VMEM(coupling.shape, BF16),
            pltpu.VMEM(solve_factor.shape, BF16),
            pltpu.VMEM((sub_count,) + near.shape, jnp.int32),
            pltpu.VMEM((sub_count,) + ownership.shape, jnp.int32),
            pltpu.VMEM((districts * LINK_COUNT, group + 2 * HALO), jnp.int32),
            pltpu.VMEM((districts, group), jnp.int32),
            pltpu.VMEM((districts, rows, interface), BF16),
            pltpu.VMEM((group, interface), BF16),
            pltpu.VMEM((group, interface), F32),
            pltpu.VMEM((group, interface), F32),
            pltpu.VMEM((group + 2 * HALO, interface), BF16),
            pltpu.VMEM((window, interface), F32),
            pltpu.VMEM((blocks, block, window), BF16),
            pltpu.VMEM((interface, interface), BF16),
            pltpu.VMEM((group, RESERVOIRS), BF16),
            pltpu.VMEM((RESERVOIRS, group), BF16),
            pltpu.VMEM((blocks, block, block), BF16),
            pltpu.VMEM((block, window), BF16),
            pltpu.VMEM((districts, rows, interface), BF16),
            pltpu.VMEM((districts, rows, interface), BF16),
            pltpu.VMEM((districts, rows, interface), F32),
            pltpu.VMEM((districts, rows, interface), F32),
            pltpu.VMEM((RESERVOIRS, LANES), F32),
            pltpu.VMEM((OUTER_ITERS, RESERVOIRS, LANES), F32),
            pltpu.VMEM((OUTER_ITERS, district_count * districts, RESERVOIRS, LANES), F32),
            dma((2 * districts + 5,)),
            dma((sub_count,)),
            dma((sub_count,)),
            dma((sub_count,)),
            dma((sub_count,)),
            dma((sub_count,)),
            dma((sub_count,)),
            dma((OUTER_ITERS, district_count * districts)),
            dma((OUTER_ITERS, district_count * districts)),
            dma((districts,)),
            dma((districts,)),
            dma((districts,)),
            dma((districts,)),
        ],
        compiler_params=pltpu.CompilerParams(
            collective_id=0, has_side_effects=True, vmem_limit_bytes=(20 if group <= 1024 else 60) * 1024 * 1024
        ),
    )(*[pltpu.with_memory_space_constraint(value, pltpu.HBM) for value in (cost_terms, near, ownership, relayout, capacity, coupling, solve_factor)])
    return pl.pallas_call(
        handover,
        name="handover",
        out_shape=tuple(jax.ShapeDtypeStruct(value.shape, value.dtype) for value in results),
        in_specs=[hbm] * 3,
        out_specs=(hbm,) * 3,
        scratch_shapes=[dma((3,))],
        compiler_params=pltpu.CompilerParams(vmem_limit_bytes=4 * 1024 * 1024),
    )(*results)


def solution(mesh):
    placed = (
        P("district", "sub", None),
        P("district", "sub", None),
        P("district", None),
        P("district", "sub"),
        P(),
        P("district", None, None),
        P("district", None, None),
    )
    return jax.shard_map(
        on_device,
        mesh=mesh,
        in_specs=placed,
        out_specs=(P("district", "sub", None), P("district", "sub", None), P()),
        check_vma=False,
    )
```

```python
import functools
import math

import jax
import jax.numpy as jnp
from jax import lax
from jax.experimental import pallas as pl
from jax.experimental.pallas import tpu as pltpu
from jax.sharding import PartitionSpec as P

REACH_SPAN = 16
LINK_COUNT = 4
RESERVOIRS = 16
OUTER_ITERS = 2
INNER_ITERS = 4
HALO = 2 * REACH_SPAN
LANES = 128

price_step = 0.3
reserve_step = 1.0

F32 = jnp.float32
BF16 = jnp.bfloat16
MESH = pl.DeviceIdType.MESH


def each(count, body):
    if count <= 8:
        for index in range(count):
            body(index)
    else:
        lax.fori_loop(0, count, lambda index, carry: (body(index), carry)[1], 0)


def mm(a, b):
    return jnp.dot(a, b, preferred_element_type=F32)


def contract(a, b, dim):
    return lax.dot_general(a, b, (((dim,), (dim,)), ((), ())), preferred_element_type=F32)


def kernel(
    dual_scale, costs_hbm, near_hbm, owner_hbm, relayout_hbm, capacity_hbm, coupling_hbm, factor_hbm,
    plan_ref, prices_ref, duals_ref,
    costs_ref, near_ref, owner_ref, relayout_ref, capacity_ref, coupling, factor, near, owned, links, owners, first, gathered, base, state, flow, total, spread, weight,
    match, match_t, select, near_links, chosen_out, chosen_in, prices_out, prices_in, duals, draws, arrived,
    local_sem, near_send, near_recv, owner_send, owner_recv, flow_send, flow_recv, draw_send, draw_recv,
    price_send, price_recv, dual_send, dual_recv,
):
    districts, rows, unknowns = costs_ref.shape
    interface = coupling.shape[1]
    horizon = capacity_ref.shape[1]
    group = relayout_ref.shape[1]
    sub_count = lax.axis_size("sub")
    district_count = lax.axis_size("district")
    me = lax.axis_index("sub")
    role = lax.rem(me, districts)
    team = me // districts * districts
    my_district = lax.axis_index("district")
    block = districts * rows
    window = block + 2 * HALO
    blocks = group // block

    costs_load = pltpu.make_async_copy(costs_hbm, costs_ref, local_sem.at[2 * districts])
    costs_load.start()
    loads = []
    for d in range(districts):
        loads.append(
            (
                pltpu.make_async_copy(factor_hbm.at[d], factor.at[d], local_sem.at[2 * d]),
                pltpu.make_async_copy(coupling_hbm.at[d], coupling.at[d], local_sem.at[2 * d + 1]),
            )
        )
        for load in loads[-1]:
            load.start()

    small_loads = [
        pltpu.make_async_copy(source, target, local_sem.at[2 * districts + 1 + index])
        for index, (source, target) in enumerate(
            (
                (near_hbm, near_ref),
                (owner_hbm, owner_ref),
                (relayout_hbm, relayout_ref),
                (capacity_hbm, capacity_ref),
            )
        )
    ]
    for load in small_loads:
        load.start()

    barrier = pltpu.get_barrier_semaphore()
    for step in range(1, sub_count):
        pl.semaphore_signal(
            barrier, inc=1, device_id={"sub": lax.rem(me + step, sub_count)}, device_id_type=MESH
        )
    for step in range(1, district_count):
        for other in range(districts):
            pl.semaphore_signal(
                barrier,
                inc=1,
                device_id={
                    "district": lax.rem(my_district + step, district_count),
                    "sub": team + lax.rem(role + other, districts),
                },
                device_id_type=MESH,
            )

    costs_load.wait()
    mine = pl.ds(pl.multiple_of(me * rows, rows), rows)
    for d in range(districts):
        for load in loads[d]:
            load.wait()
        first_plan = -mm(costs_ref[d], factor[d])
        first[d] = contract(first_plan.astype(BF16), coupling[d], 1).astype(BF16)

    for load in small_loads:
        load.wait()
    pl.semaphore_wait(barrier, sub_count - 1 + (district_count - 1) * districts)
    sends = []
    for step in range(1, sub_count):
        target = lax.rem(me + step, sub_count)
        for source_ref, place_ref, send_sem, recv_sem in (
            (near_ref, near, near_send, near_recv),
            (owner_ref, owned, owner_send, owner_recv),
        ):
            sends.append(
                pltpu.make_async_remote_copy(
                    src_ref=source_ref,
                    dst_ref=place_ref.at[me],
                    send_sem=send_sem.at[step],
                    recv_sem=recv_sem.at[me],
                    device_id={"sub": target},
                    device_id_type=MESH,
                )
            )
            sends[-1].start()
    for step in sorted(range(1, sub_count), key=lambda step: abs(2 * step - sub_count)):
        target = lax.rem(me + step, sub_count)
        sends.append(
            pltpu.make_async_remote_copy(
                src_ref=first.at[lax.rem(target, districts)],
                dst_ref=gathered.at[mine, :],
                send_sem=flow_send.at[step],
                recv_sem=flow_recv.at[me],
                device_id={"sub": target},
                device_id_type=MESH,
            )
        )
        sends[-1].start()

    gathered[mine, :] = first[role]
    narrow = mm(coupling[role], factor[role]).astype(BF16)
    weight[...] = (-contract(narrow, coupling[role], 1)).astype(BF16)

    wide = rows + 2 * HALO
    moves = relayout_ref[pl.ds(role, 1), :]
    team_rows = districts * rows
    pick = lax.broadcasted_iota(jnp.int32, (team_rows, group), 1) == (
        lax.broadcasted_iota(jnp.int32, (team_rows, group), 0) + team * rows
    )
    pick = jnp.where(pick, 1.0, 0.0).astype(BF16)

    def choose(b):
        place = lax.broadcasted_iota(jnp.int32, (block, group), 0) + b * block
        chosen = jnp.where(place == moves, 1.0, 0.0).astype(BF16)
        select[b] = contract(pick, chosen, 1).astype(BF16)

    each(blocks, choose)

    duals[...] = jnp.zeros_like(duals)
    duals[:, :horizon] = capacity_ref[...]
    capacity = duals[...]
    flow[...] = jnp.zeros_like(flow)
    links[...] = jnp.full_like(links, -window * 4)

    near[me] = near_ref[...]
    owned[me] = owner_ref[...]
    for step in range(1, sub_count):
        source = lax.rem(me + step, sub_count)
        for source_ref, place_ref, send_sem, recv_sem in (
            (near_ref, near, near_send, near_recv),
            (owner_ref, owned, owner_send, owner_recv),
        ):
            pltpu.make_async_remote_copy(
                src_ref=source_ref,
                dst_ref=place_ref.at[source],
                send_sem=send_sem.at[step],
                recv_sem=recv_sem.at[source],
                device_id={"sub": source},
                device_id_type=MESH,
            ).wait_recv()
    for source in range(sub_count):
        links[:, HALO + source * rows : HALO + (source + 1) * rows] = near[source]
        owners[:, source * rows : (source + 1) * rows] = owned[source]
    own = owners[pl.ds(role, 1), :]
    hit = jnp.where(
        lax.broadcasted_iota(jnp.int32, (RESERVOIRS, group), 0) == own, 1.0, 0.0
    ).astype(F32)
    match_t[...] = hit.astype(BF16)
    match[...] = hit.T.astype(BF16)

    def linked(start, width):
        column = lax.broadcasted_iota(jnp.int32, (width, width), 0)
        row = lax.broadcasted_iota(jnp.int32, (width, width), 1)
        table = jnp.where(column == row, 1.0, 0.0)
        for k in range(LINK_COUNT):
            link = links[pl.ds(role * LINK_COUNT + k, 1), pl.ds(start, width)] - (start - HALO)
            table = table - jnp.where(column == link, 1.0 / LINK_COUNT, 0.0)
        return table.T.astype(BF16)

    def build(b):
        start = b * block if isinstance(b, int) else pl.multiple_of(b * block, block)
        table = linked(start, window)
        spread[b] = mm(table[HALO : HALO + block], table).astype(BF16)

    each(blocks, build)
    near_links[...] = linked(pl.multiple_of(team * rows, team_rows), window)[HALO : HALO + team_rows]

    for step in range(1, sub_count):
        source = lax.rem(me + step, sub_count)
        pltpu.make_async_remote_copy(
            src_ref=first.at[role],
            dst_ref=gathered.at[pl.ds(pl.multiple_of(source * rows, rows), rows), :],
            send_sem=flow_send.at[step],
            recv_sem=flow_recv.at[source],
            device_id={"sub": source},
            device_id_type=MESH,
        ).wait_recv()

    def at_block(b, extra=0, size=block):
        return pl.ds(b * block + extra, size)

    def permute(b):
        place = lax.broadcasted_iota(jnp.int32, (block, group), 0) + b * block
        chosen = jnp.where(place == moves, 1.0, 0.0).astype(BF16)
        moved = mm(chosen, gathered[...])
        base[at_block(b), :] = moved
        flow[at_block(b, HALO), :] = moved.astype(BF16)

    each(blocks, permute)

    team_window = pl.ds(pl.multiple_of(team * rows, team_rows), window)
    total[...] = flow[team_window, :].astype(F32)

    def begin(b):
        state[at_block(b), :] = price_step * mm(spread[b], flow[at_block(b, 0, window), :])

    each(blocks, begin)

    def forward():
        def one(b):
            price = state[at_block(b), :].astype(BF16)
            flow[at_block(b, HALO), :] = (base[at_block(b), :] + mm(price, weight[...])).astype(BF16)

        each(blocks, one)
        total[...] += flow[team_window, :].astype(F32)

    def backward():
        def one(b):
            state[at_block(b), :] += price_step * mm(spread[b], flow[at_block(b, 0, window), :])

        each(blocks, one)

    def inner(step, carry):
        forward()
        backward()
        return carry

    partners = [
        (step, other)
        for step in range(district_count)
        for other in range(districts)
        if step or other
    ]

    def partner(step, other):
        return {
            "district": lax.rem(my_district + step, district_count),
            "sub": team + lax.rem(role + other, districts),
        }

    def send_draws(outer):
        drawn = mm(match_t[...], flow[HALO : HALO + group, :])
        draws[outer] = drawn[:, :LANES]
        copies = []
        for index, (step, other) in enumerate(partners):
            copies.append(
                pltpu.make_async_remote_copy(
                    src_ref=draws.at[outer],
                    dst_ref=arrived.at[outer, index],
                    send_sem=draw_send.at[outer, index],
                    recv_sem=draw_recv.at[outer, index],
                    device_id=partner(step, other),
                    device_id_type=MESH,
                )
            )
            copies[-1].start()
        return copies

    def take_draws(outer, copies):
        drawn = draws[outer]
        for index, copy in enumerate(copies):
            copy.wait()
            drawn = drawn + arrived[outer, index]
        lane = lax.broadcasted_iota(jnp.int32, drawn.shape, 1)
        return jnp.where(lane < horizon, (drawn - capacity) * dual_scale, 0.0)

    def to_team(source_ref, place_ref, send_sem, recv_sem):
        copies = []
        for other in range(1, districts):
            target = lax.rem(role + other, districts)
            copies.append(
                pltpu.make_async_remote_copy(
                    src_ref=source_ref.at[target],
                    dst_ref=place_ref.at[role],
                    send_sem=send_sem.at[other],
                    recv_sem=recv_sem.at[other],
                    device_id={"sub": team + target},
                    device_id_type=MESH,
                )
            )
            copies[-1].start()
        return copies

    lax.fori_loop(1, INNER_ITERS - 1, inner, 0)
    forward()
    copies = send_draws(0)
    backward()
    moved = take_draws(0, copies)
    for outer in range(1, OUTER_ITERS):
        duals[...] = moved if outer == 1 else duals[...] + moved
        high = moved.astype(BF16)
        low = (moved - high.astype(F32)).astype(BF16)
        state[:, :LANES] += mm(match[...], high) + mm(match[...], low)
        lax.fori_loop(0, INNER_ITERS - 1, inner, 0)
        if outer == OUTER_ITERS - 1:
            price = state[...].astype(BF16)
            chosen = mm(select[0], price[:block])
            for b in range(1, blocks):
                chosen = chosen + mm(select[b], price[b * block : (b + 1) * block])
            chosen_out[...] = chosen.reshape(districts, rows, -1).astype(BF16)
            price_copies = to_team(chosen_out, chosen_in, price_send, price_recv)
            chosen_in[role] = chosen_out[role]
        forward()
        copies = send_draws(outer)
        if outer < OUTER_ITERS - 1:
            backward()
        else:
            high = total[...].astype(BF16)
            low = (total[...] - high.astype(F32)).astype(BF16)
            prices = price_step * (mm(near_links[...], high) + mm(near_links[...], low))
            prices_out[...] = prices.reshape(districts, rows, -1)
            dual_copies = to_team(prices_out, prices_in, dual_send, dual_recv)
            prices_in[role] = prices_out[role]
            for copy in price_copies:
                copy.wait()
            for d in range(districts):
                gradient = costs_ref[d].astype(F32) + mm(chosen_in[d], coupling[d])
                plan_ref[d] = -mm(gradient.astype(BF16), factor[d])
            for copy in dual_copies:
                copy.wait()
            prices_ref[...] = prices_in[...]
        moved = take_draws(outer, copies)
    duals_ref[...] = (duals[...] + moved)[:, :horizon]
    for send in sends:
        send.wait_send()


def handover(plan_ref, prices_ref, duals_ref, plan_out, prices_out, duals_out, sem):
    copies = [
        pltpu.make_async_copy(source, target, sem.at[index])
        for index, (source, target) in enumerate(
            ((plan_ref, plan_out), (prices_ref, prices_out), (duals_ref, duals_out))
        )
    ]
    for copy in copies:
        copy.start()
    for copy in copies:
        copy.wait()


def on_device(cost_terms, neighbours, relayout, ownership, capacity, coupling, solve_factor):
    districts, rows, unknowns = cost_terms.shape
    interface = coupling.shape[2]
    group = relayout.shape[1]
    sub_count = lax.axis_size("sub")
    district_count = lax.axis_size("district")
    load_count = districts * district_count * group // (2 * RESERVOIRS)
    dual_scale = reserve_step / math.sqrt(load_count)
    near = neighbours.transpose(0, 2, 1).reshape(districts * LINK_COUNT, rows)
    coupling = coupling.transpose(0, 2, 1)
    block = districts * rows
    blocks = group // block
    window = block + 2 * HALO
    vmem = pl.BlockSpec(memory_space=pltpu.VMEM)
    hbm = pl.BlockSpec(memory_space=pl.ANY)
    dma = pltpu.SemaphoreType.DMA
    results = pl.pallas_call(
        functools.partial(kernel, dual_scale),
        name="districts",
        out_shape=(
            jax.ShapeDtypeStruct((districts, rows, unknowns), F32),
            jax.ShapeDtypeStruct((districts, rows, interface), F32),
            jax.ShapeDtypeStruct(capacity.shape, F32),
        ),
        in_specs=[pl.BlockSpec(memory_space=pltpu.HBM)] * 7,
        out_specs=(vmem, vmem, vmem),
        scratch_shapes=[
            pltpu.VMEM(cost_terms.shape, BF16),
            pltpu.VMEM(near.shape, jnp.int32),
            pltpu.VMEM(ownership.shape, jnp.int32),
            pltpu.VMEM(relayout.shape, jnp.int32),
            pltpu.VMEM(capacity.shape, F32),
            pltpu.VMEM(coupling.shape, BF16),
            pltpu.VMEM(solve_factor.shape, BF16),
            pltpu.VMEM((sub_count,) + near.shape, jnp.int32),
            pltpu.VMEM((sub_count,) + ownership.shape, jnp.int32),
            pltpu.VMEM((districts * LINK_COUNT, group + 2 * HALO), jnp.int32),
            pltpu.VMEM((districts, group), jnp.int32),
            pltpu.VMEM((districts, rows, interface), BF16),
            pltpu.VMEM((group, interface), BF16),
            pltpu.VMEM((group, interface), F32),
            pltpu.VMEM((group, interface), F32),
            pltpu.VMEM((group + 2 * HALO, interface), BF16),
            pltpu.VMEM((window, interface), F32),
            pltpu.VMEM((blocks, block, window), BF16),
            pltpu.VMEM((interface, interface), BF16),
            pltpu.VMEM((group, RESERVOIRS), BF16),
            pltpu.VMEM((RESERVOIRS, group), BF16),
            pltpu.VMEM((blocks, block, block), BF16),
            pltpu.VMEM((block, window), BF16),
            pltpu.VMEM((districts, rows, interface), BF16),
            pltpu.VMEM((districts, rows, interface), BF16),
            pltpu.VMEM((districts, rows, interface), F32),
            pltpu.VMEM((districts, rows, interface), F32),
            pltpu.VMEM((RESERVOIRS, LANES), F32),
            pltpu.VMEM((OUTER_ITERS, RESERVOIRS, LANES), F32),
            pltpu.VMEM((OUTER_ITERS, district_count * districts, RESERVOIRS, LANES), F32),
            dma((2 * districts + 5,)),
            dma((sub_count,)),
            dma((sub_count,)),
            dma((sub_count,)),
            dma((sub_count,)),
            dma((sub_count,)),
            dma((sub_count,)),
            dma((OUTER_ITERS, district_count * districts)),
            dma((OUTER_ITERS, district_count * districts)),
            dma((districts,)),
            dma((districts,)),
            dma((districts,)),
            dma((districts,)),
        ],
        compiler_params=pltpu.CompilerParams(
            collective_id=0, has_side_effects=True, vmem_limit_bytes=(20 if group <= 1024 else 60) * 1024 * 1024
        ),
    )(*[pltpu.with_memory_space_constraint(value, pltpu.HBM) for value in (cost_terms, near, ownership, relayout, capacity, coupling, solve_factor)])
    return pl.pallas_call(
        handover,
        name="handover",
        out_shape=tuple(jax.ShapeDtypeStruct(value.shape, value.dtype) for value in results),
        in_specs=[hbm] * 3,
        out_specs=(hbm,) * 3,
        scratch_shapes=[dma((3,))],
        compiler_params=pltpu.CompilerParams(vmem_limit_bytes=4 * 1024 * 1024),
    )(*results)


def solution(mesh):
    placed = (
        P("district", "sub", None),
        P("district", "sub", None),
        P("district", None),
        P("district", "sub"),
        P(),
        P("district", None, None),
        P("district", None, None),
    )
    return jax.shard_map(
        on_device,
        mesh=mesh,
        in_specs=placed,
        out_specs=(P("district", "sub", None), P("district", "sub", None), P()),
        check_vma=False,
    )
```
